32 devices in a mesh: dp: 4 (over y, core), expert: 4 (over z), tensor: 2 (over x).
Axes of the slice: x: 2, y: 2, z: 4, core: 2. Of those that a mesh axis runs over, the one named last changes fastest.
Arguments:
- tokens: bfloat16 [1024, 3584], P(('dp', 'expert'), 'tensor'), may hold values from -6 to 6
- route_slots: int32 [1024, 8], P(('dp', 'expert')), may hold values from 0 to 15, as said below
- route_scores: float32 [1024, 8], P(('dp', 'expert')), may hold values from 0.05 to 1
- slot_expert: int32 [16], replicated, may hold values from 0 to 11, as said below
- w_in: bfloat16 [16, 3584, 2, 1024], P('expert', None, None, 'tensor'), may hold values from -6 to 6, as said below
- w_out: bfloat16 [16, 1024, 3584], P('expert', 'tensor'), may hold values from -6 to 6, as said below
Outputs:
- moe_out: bfloat16 [1024, 3584], P(('dp', 'expert'), 'tensor')
- expert_load: float32 [4, 12], P('dp')
The draws below stay inside these ranges and needn't reach their ends.
Inputs may be any that keep to these rules, and one draw needn't show every extreme that they name: `route_slots`: each row names 8 different slots. In each device's block of 64 rows no slot is named by more than 36 rows, and one slot is named by exactly 36 rows in every block. `slot_expert`: every expert is held by one or two slots; 4 experts are held by two. `w_in`: slots that hold the same expert hold equal weights. `w_out`: slots that hold the same expert hold equal weights.
All inputs are finite; a program needn't handle non-finite values.
Results may differ from the reference program's by a relative error of at most 0.012.
Values may be sent and summed in bfloat16 or wider, within the bound.
No kernel may reach another device: no remote copies, remote signals or barrier semaphores. Data moves between devices by JAX's collectives and lax.ppermute only.
A program may use at most 128 MiB of HBM per device.

```python
import math
import jax
import jax.numpy as jnp
from jax import lax

D = 3584
F = 1024
TOP = 8
TOK_DEV = 64
SLOTS = 16
SPARE = 4
EXPERTS = 12
CAP = 36
TOKENS = 1024
N_DP = 4
N_EXPERT = 4
N_TENSOR = 2


def placement_table(key):
    base = jax.random.fold_in(key, 7)
    order = jax.random.permutation(jax.random.fold_in(base, 1), SLOTS)
    copied = jax.random.permutation(jax.random.fold_in(base, 2), EXPERTS)[:SPARE]
    held = jnp.concatenate([jnp.arange(EXPERTS, dtype=jnp.int32), copied.astype(jnp.int32)])
    return jnp.zeros((SLOTS,), jnp.int32).at[order].set(held)


def draw_slot_expert(key, part):
    return placement_table(key)


def draw_w_in(key, part):
    holder = placement_table(key)
    base = jax.random.fold_in(key, 101)

    def one_slot(expert_id):
        values = jax.random.normal(jax.random.fold_in(base, expert_id), (D, 2, F), jnp.float32)
        return (jnp.clip(values, -6.0, 6.0) * D ** (-0.5)).astype(jnp.bfloat16)
    return lax.map(one_slot, holder)


def draw_w_out(key, part):
    holder = placement_table(key)
    base = jax.random.fold_in(key, 202)

    def one_slot(expert_id):
        values = jax.random.normal(jax.random.fold_in(base, expert_id), (F, D), jnp.float32)
        return (jnp.clip(values, -6.0, 6.0) * F ** (-0.5)).astype(jnp.bfloat16)
    return lax.map(one_slot, holder)


def draw_route_slots(key, part):
    rank_key = jax.random.fold_in(key, 31)
    hot_key = jax.random.fold_in(key, 32)
    block_key = jax.random.fold_in(key, 33)
    ranking = jax.random.permutation(rank_key, SLOTS).astype(jnp.int32)
    hottest = jax.random.randint(hot_key, (), 0, SLOTS)
    pool_slot = jnp.repeat(jnp.arange(SLOTS, dtype=jnp.int32), CAP)
    pool_index = jnp.arange(SLOTS * CAP, dtype=jnp.int32)

    def one_block(block_seed):
        noise_key, row_key = jax.random.split(block_seed)
        noise = jax.random.randint(noise_key, (SLOTS * CAP,), 0, 32 * SLOTS)
        scores = noise + 16 * ranking[pool_slot]
        scores = jnp.where(pool_slot == hottest, -1, scores)
        order = jnp.argsort(scores * (SLOTS * CAP) + pool_index, stable=True)
        chosen = jnp.sort(pool_slot[order[:TOK_DEV * TOP]])
        layout = chosen.reshape(TOP, TOK_DEV).T
        shuffle = jax.random.permutation(row_key, TOK_DEV)
        return layout[shuffle]
    seeds = jax.random.split(block_key, TOKENS // TOK_DEV)
    return jax.vmap(one_block)(seeds).reshape(TOKENS, TOP).astype(jnp.int32)


def steps_of(rng, extent, cuts, least, top_value):
    def one(dim, parts):
        draws = jax.random.uniform(jax.random.fold_in(jax.random.fold_in(rng, 6), dim), (parts,), jnp.float32, least / len(cuts), top_value / len(cuts))
        return jnp.repeat(jnp.exp(draws), extent[dim] // parts).reshape((-1,) + (1,) * (len(extent) - dim - 1))

    gain = one(*cuts[0])
    for cut in cuts[1:]:
        gain = gain * one(*cut)
    return gain


def bell_draw(own_key, dims, deviation, reach, shards=(), kind=jnp.bfloat16):
    values = deviation * jax.random.normal(own_key, dims, jnp.float32)
    if shards:
        values = values * steps_of(own_key, dims, shards, -0.22, 0.18)
    return jnp.clip(values, -reach, reach).astype(kind)


def setup_inputs(seed: int = 0) -> dict:
    splits = jax.random.split(jax.random.key(seed), 7)
    return {
        "tokens": bell_draw(splits[0], (TOKENS, D), 1.0, 6.0, ((0, 16), (1, 2))),
        "route_slots": draw_route_slots(jax.random.fold_in(splits[6], 71), 0),
        "route_scores": jnp.clip(jnp.exp(math.log(1.0) - 2.9957323 * jax.random.uniform(splits[2], (TOKENS, TOP), jnp.float32) ** steps_of(splits[2], (TOKENS, TOP), ((0, 16),), -0.2, 0.2)), 0.05, 1.0),
        "slot_expert": draw_slot_expert(jax.random.fold_in(splits[6], 71), 0),
        "w_in": draw_w_in(jax.random.fold_in(splits[6], 71), 0),
        "w_out": draw_w_out(jax.random.fold_in(splits[6], 71), 0),
    }


ROUTED = 2.5


def reference(tokens, route_slots, route_scores, slot_expert, w_in, w_out):
    gates = route_scores / jnp.sum(route_scores, axis=1, keepdims=True) * ROUTED
    flat_slot = route_slots.reshape(-1)
    flat_gate = gates.reshape(-1)
    token_of = (jnp.arange(TOKENS * TOP, dtype=jnp.int32) // TOP).astype(jnp.int32)
    most_rows = N_DP * N_EXPERT * CAP
    part_units = F // N_TENSOR

    def one_slot(running, slot_id):
        chosen = flat_slot == slot_id
        position = jnp.cumsum(chosen.astype(jnp.int32)) - 1
        landing = jnp.where(chosen, position, most_rows).astype(jnp.int32)
        picked = jnp.zeros((most_rows,), jnp.int32).at[landing].set(token_of, mode="drop")
        weight = jnp.zeros((most_rows,), jnp.float32).at[landing].set(flat_gate, mode="drop")
        gathered = tokens[picked]
        w_first = w_in[slot_id].reshape(D, 2 * F)
        projected = jnp.dot(gathered, w_first, preferred_element_type=jnp.float32).reshape(most_rows, 2, F)
        hidden = (jax.nn.silu(projected[:, 0]) * projected[:, 1]).astype(jnp.bfloat16)
        w_second = w_out[slot_id]
        summed = jnp.zeros((most_rows, D), jnp.float32)
        for tensor_part in range(N_TENSOR):
            first_unit = tensor_part * part_units
            partial_value = jnp.dot(hidden[:, first_unit:first_unit + part_units], w_second[first_unit:first_unit + part_units], preferred_element_type=jnp.float32)
            rounded = lax.optimization_barrier(partial_value.astype(jnp.bfloat16))
            summed = summed + rounded.astype(jnp.float32)
        expert_out = lax.optimization_barrier(summed.astype(jnp.bfloat16))
        running = running.at[picked].add(weight[:, None] * expert_out.astype(jnp.float32))
        return running, None

    running, unused = lax.scan(one_slot, jnp.zeros((TOKENS, D), jnp.float32), jnp.arange(SLOTS, dtype=jnp.int32))
    moe_out = running.astype(jnp.bfloat16)
    matches = route_slots.reshape(N_DP, -1)[:, :, None] == jnp.arange(SLOTS, dtype=jnp.int32)[None, None, :]
    slot_totals = jnp.sum(jnp.where(matches, gates.reshape(N_DP, -1)[:, :, None], 0.0), axis=1)
    holder = (slot_expert[:, None] == jnp.arange(EXPERTS, dtype=jnp.int32)[None, :]).astype(jnp.float32)
    expert_load = jnp.sum(slot_totals[:, :, None] * holder[None], axis=1) * (EXPERTS / (N_EXPERT * TOK_DEV * ROUTED))
    return moe_out, expert_load
```

```python
import jax
import jax.numpy as jnp
from jax import lax
from jax.sharding import PartitionSpec as P

ROUTED = 2.5


def routed_plan(tokens, route_slots, route_scores, slot_expert, w_in, w_out):
    tok_rows, piece_cols = tokens.shape
    choices = route_slots.shape[1]
    slot_local = w_in.shape[0]
    owners = lax.axis_size("expert")
    slot_count = slot_local * owners
    capacity = 9 * tok_rows * choices // (8 * slot_count)
    experts = slot_count - slot_count // 4
    weights_of = route_scores / jnp.sum(route_scores, axis=1, keepdims=True) * ROUTED
    flat_slot = route_slots.reshape(-1)
    matches = flat_slot[:, None] == jnp.arange(slot_count, dtype=jnp.int32)[None, :]
    counted = jnp.cumsum(matches.astype(jnp.int32), axis=0)
    ranking = jnp.sum(jnp.where(matches, counted, 0), axis=1) - 1
    target = flat_slot * capacity + ranking
    row_of = jnp.arange(tok_rows * choices, dtype=jnp.int32) // choices
    source = jnp.full((slot_count * capacity,), tok_rows, jnp.int32).at[target].set(row_of)
    slot_sums = jnp.sum(jnp.where(matches, weights_of.reshape(-1)[:, None], 0.0), axis=0)
    totals = lax.psum(slot_sums, "expert")
    padded = jnp.concatenate([tokens, jnp.zeros((1, piece_cols), tokens.dtype)], axis=0)
    outgoing = jnp.take(padded, source, axis=0).reshape(owners, slot_local * capacity, piece_cols)
    arrived = lax.all_to_all(outgoing, "expert", split_axis=0, concat_axis=0, tiled=True)
    arrived = arrived.reshape(owners, slot_local, capacity, piece_cols)
    assembled = lax.all_gather(arrived, "tensor", axis=3, tiled=True)
    projected = jnp.einsum("nscd,sdgf->nscgf", assembled, w_in, preferred_element_type=jnp.float32)
    hidden = (jax.nn.silu(projected[:, :, :, 0]) * projected[:, :, :, 1]).astype(jnp.bfloat16)
    partial_value = jnp.einsum("nscf,sfd->nscd", hidden, w_out, preferred_element_type=jnp.float32)
    summed = lax.psum_scatter(
        partial_value.astype(jnp.bfloat16), "tensor", scatter_dimension=3, tiled=True
    )
    results = summed.reshape(owners, slot_local * capacity, piece_cols)
    returned = lax.all_to_all(results, "expert", split_axis=0, concat_axis=0, tiled=True)
    returned = returned.reshape(slot_count * capacity, piece_cols)
    picked = jnp.take(returned, target, axis=0).reshape(tok_rows, choices, piece_cols)
    moe_out = jnp.sum(picked.astype(jnp.float32) * weights_of[:, :, None], axis=1).astype(
        jnp.bfloat16
    )
    holder = (slot_expert[:, None] == jnp.arange(experts, dtype=jnp.int32)[None, :]).astype(
        jnp.float32
    )
    expert_load = jnp.sum(totals[:, None] * holder, axis=0) * (
        experts / (owners * tok_rows * ROUTED)
    )
    return (moe_out, expert_load[None, :])


def swap(value, axis, bit):
    size = lax.axis_size(axis)
    return lax.ppermute(value, axis, [(i, i ^ bit) for i in range(size)])


def bits_of(axis):
    size = lax.axis_size(axis)
    return [1 << b for b in reversed(range(size.bit_length() - 1))]


def gathered(value, axis):
    chunks = {0: value}
    for bit in bits_of(axis):
        for mask in list(chunks):
            chunks[mask | bit] = swap(chunks[mask], axis, bit)
    return [chunks[i] for i in range(len(chunks))]


def scattered(chunks, axis):
    left = dict(enumerate(chunks))
    for bit in reversed(bits_of(axis)):
        for mask in list(left):
            if mask & bit:
                sent = swap(left.pop(mask), axis, bit)
                other = left[mask ^ bit]
                left[mask ^ bit] = (
                    other.astype(jnp.float32) + sent.astype(jnp.float32)
                ).astype(sent.dtype)
    return left[0]


def pair_sum(items):
    items = list(items)
    while len(items) > 1:
        items = [a + b for a, b in zip(items[::2], items[1::2])]
    return items[0]


def gathered_plan(tokens, route_slots, route_scores, slot_expert, w_in, w_out):
    tok_rows, piece_cols = tokens.shape
    choices = route_slots.shape[1]
    slot_local = w_in.shape[0]
    owners = lax.axis_size("expert")
    slot_count = slot_local * owners
    experts = slot_count - slot_count // 4
    side = lax.axis_index("tensor")
    first_slot = lax.axis_index("expert") * slot_local
    weights_of = route_scores / jnp.sum(route_scores, axis=1, keepdims=True) * ROUTED
    info = jnp.concatenate([route_slots.astype(jnp.float32), weights_of], axis=1)
    mine = gathered(tokens, "expert")
    infos = gathered(info, "expert")
    theirs = [swap(v, "tensor", 1) for v in mine]
    near, far = jnp.concatenate(mine, axis=0), jnp.concatenate(theirs, axis=0)
    whole = jnp.concatenate(
        [jnp.where(side == 0, near, far), jnp.where(side == 0, far, near)], axis=1
    )
    slots_f = jnp.concatenate(infos, axis=0)
    slots, weights = slots_f[:, :choices].astype(jnp.int32), slots_f[:, choices:]
    every = jnp.arange(slot_count, dtype=jnp.int32)
    gates = jnp.sum(
        jnp.where(slots[:, :, None] == every[None, None, :], weights[:, :, None], 0.0), axis=1
    )
    totals = pair_sum(jnp.sum(gates.reshape(owners, tok_rows, slot_count), axis=1))
    local = lax.dynamic_slice_in_dim(gates, first_slot, slot_local, axis=1)
    projected = jnp.einsum("td,sdgf->tsgf", whole, w_in, preferred_element_type=jnp.float32)
    hidden = jax.nn.silu(projected[:, :, 0]) * projected[:, :, 1] * local[:, :, None]
    partial_value = jnp.einsum(
        "tsf,sfd->td", hidden.astype(jnp.bfloat16), w_out, preferred_element_type=jnp.float32
    ).astype(jnp.bfloat16)
    keep = lax.dynamic_slice_in_dim(partial_value, side * piece_cols, piece_cols, axis=1)
    give = lax.dynamic_slice_in_dim(partial_value, (1 - side) * piece_cols, piece_cols, axis=1)
    pieces = []
    for i in range(owners):
        rows = slice(i * tok_rows, (i + 1) * tok_rows)
        got = swap(give[rows], "tensor", 1)
        pieces.append(
            (keep[rows].astype(jnp.float32) + got.astype(jnp.float32)).astype(jnp.bfloat16)
        )
    moe_out = scattered(pieces, "expert")
    holder = (slot_expert[:, None] == jnp.arange(experts, dtype=jnp.int32)[None, :]).astype(
        jnp.float32
    )
    expert_load = jnp.sum(totals[:, None] * holder, axis=0) * (
        experts / (owners * tok_rows * ROUTED)
    )
    return (moe_out, expert_load[None, :])


def shards(*args):
    tokens, route_slots, w_in = args[0], args[1], args[4]
    owners = lax.axis_size("expert")
    slot_count = w_in.shape[0] * owners
    capacity = 9 * tokens.shape[0] * route_slots.shape[1] // (8 * slot_count)
    dense = w_in.shape[0] * capacity >= tokens.shape[0]
    paired = owners & (owners - 1) == 0 and lax.axis_size("tensor") == 2
    return (gathered_plan if dense and paired else routed_plan)(*args)


def solution(mesh):
    placed = (
        P(("dp", "expert"), "tensor"),
        P(("dp", "expert"), None),
        P(("dp", "expert"), None),
        P(),
        P("expert", None, None, "tensor"),
        P("expert", "tensor", None),
    )
    return jax.shard_map(
        shards,
        mesh=mesh,
        in_specs=placed,
        out_specs=(P(("dp", "expert"), "tensor"), P("dp", None)),
        check_vma=False,
    )
```

```python
import jax
import jax.numpy as jnp
from jax import lax
from jax.experimental import pallas as pl
from jax.experimental.pallas import tpu as pltpu
from jax.sharding import PartitionSpec as P

ROUTED = 2.5


def routed_plan(tokens, route_slots, route_scores, slot_expert, w_in, w_out):
    tok_rows, piece_cols = tokens.shape
    choices = route_slots.shape[1]
    slot_local = w_in.shape[0]
    owners = lax.axis_size("expert")
    slot_count = slot_local * owners
    capacity = 9 * tok_rows * choices // (8 * slot_count)
    experts = slot_count - slot_count // 4
    weights_of = route_scores / jnp.sum(route_scores, axis=1, keepdims=True) * ROUTED
    flat_slot = route_slots.reshape(-1)
    matches = flat_slot[:, None] == jnp.arange(slot_count, dtype=jnp.int32)[None, :]
    counted = jnp.cumsum(matches.astype(jnp.int32), axis=0)
    ranking = jnp.sum(jnp.where(matches, counted, 0), axis=1) - 1
    target = flat_slot * capacity + ranking
    row_of = jnp.arange(tok_rows * choices, dtype=jnp.int32) // choices
    source = jnp.full((slot_count * capacity,), tok_rows, jnp.int32).at[target].set(row_of)
    slot_sums = jnp.sum(jnp.where(matches, weights_of.reshape(-1)[:, None], 0.0), axis=0)
    totals = lax.psum(slot_sums, "expert")
    padded = jnp.concatenate([tokens, jnp.zeros((1, piece_cols), tokens.dtype)], axis=0)
    outgoing = jnp.take(padded, source, axis=0).reshape(owners, slot_local * capacity, piece_cols)
    arrived = lax.all_to_all(outgoing, "expert", split_axis=0, concat_axis=0, tiled=True)
    arrived = arrived.reshape(owners, slot_local, capacity, piece_cols)
    assembled = lax.all_gather(arrived, "tensor", axis=3, tiled=True)
    projected = jnp.einsum("nscd,sdgf->nscgf", assembled, w_in, preferred_element_type=jnp.float32)
    hidden = (jax.nn.silu(projected[:, :, :, 0]) * projected[:, :, :, 1]).astype(jnp.bfloat16)
    partial_value = jnp.einsum("nscf,sfd->nscd", hidden, w_out, preferred_element_type=jnp.float32)
    summed = lax.psum_scatter(
        partial_value.astype(jnp.bfloat16), "tensor", scatter_dimension=3, tiled=True
    )
    results = summed.reshape(owners, slot_local * capacity, piece_cols)
    returned = lax.all_to_all(results, "expert", split_axis=0, concat_axis=0, tiled=True)
    returned = returned.reshape(slot_count * capacity, piece_cols)
    picked = jnp.take(returned, target, axis=0).reshape(tok_rows, choices, piece_cols)
    moe_out = jnp.sum(picked.astype(jnp.float32) * weights_of[:, :, None], axis=1).astype(
        jnp.bfloat16
    )
    holder = (slot_expert[:, None] == jnp.arange(experts, dtype=jnp.int32)[None, :]).astype(
        jnp.float32
    )
    expert_load = jnp.sum(totals[:, None] * holder, axis=0) * (
        experts / (owners * tok_rows * ROUTED)
    )
    return (moe_out, expert_load[None, :])


LANES = 128
WORK_ROWS = 64
WORK_SLOTS = 4


def swap(value, axis, bit):
    size = lax.axis_size(axis)
    return lax.ppermute(value, axis, [(i, i ^ bit) for i in range(size)])


def bits_of(axis):
    size = lax.axis_size(axis)
    return [1 << b for b in reversed(range(size.bit_length() - 1))]


def gathered(value, axis):
    chunks = {0: value}
    for bit in bits_of(axis):
        for mask in list(chunks):
            chunks[mask | bit] = swap(chunks[mask], axis, bit)
    return [chunks[i] for i in range(len(chunks))]


def local_call(body, out_shape, name, limit=8 << 20, in_specs=None, scratch=()):
    def call(*args):
        specs = in_specs or [pl.BlockSpec(memory_space=pltpu.VMEM)] * len(args)
        outs = jax.tree.map(lambda _: pl.BlockSpec(memory_space=pltpu.VMEM), out_shape)
        return pl.pallas_call(
            body,
            in_specs=specs,
            out_specs=outs,
            out_shape=out_shape,
            scratch_shapes=scratch,
            compiler_params=pltpu.CompilerParams(vmem_limit_bytes=limit),
            name=name,
        )(*args)

    return call


def packed_routes(slots_t, scores_t):
    choices, rows = slots_t.shape

    def body(slot_ref, score_ref, out_ref):
        scores = score_ref[...]
        out_ref[:choices] = slot_ref[...].astype(jnp.float32)
        out_ref[choices:] = scores / jnp.sum(scores, axis=0, keepdims=True) * ROUTED

    shape = jax.ShapeDtypeStruct((2 * choices, rows), jnp.float32)
    return local_call(body, shape, "routes", 1 << 20)(slots_t, scores_t)


def gates_and_load(infos, slot_expert, slot_local):
    owners = len(infos)
    choices, rows = infos[0].shape[0] // 2, infos[0].shape[1]
    slot_count = slot_expert.shape[0]
    experts = slot_count - slot_count // 4
    scale = experts / (owners * rows * ROUTED)
    padded = -(-slot_local // 8) * 8

    def body(*refs):
        expert_ref, gate_ref, load_ref = refs[owners:]
        first = lax.axis_index("expert") * slot_local
        ids = lax.broadcasted_iota(jnp.int32, (slot_count, rows), 0).astype(jnp.float32)
        locals_ = lax.broadcasted_iota(jnp.int32, (padded, rows), 0) + first
        locals_ = locals_.astype(jnp.float32)
        totals = []
        for i in range(owners):
            every = jnp.zeros((slot_count, rows), jnp.float32)
            mine = jnp.zeros((padded, rows), jnp.float32)
            for k in range(choices):
                slot = refs[i][k : k + 1, :]
                weight = refs[i][choices + k : choices + k + 1, :]
                every = every + jnp.where(slot == ids, weight, 0.0)
                mine = mine + jnp.where(slot == locals_, weight, 0.0)
            totals.append(jnp.sum(every, axis=1, keepdims=True))
            gate_ref[i * rows : (i + 1) * rows, :] = mine.T
        while len(totals) > 1:
            totals = [p + q for p, q in zip(totals[::2], totals[1::2])]
        lane = lax.broadcasted_iota(jnp.int32, (1, experts), 1)
        load = jnp.zeros((1, experts), jnp.float32)
        for s in range(slot_count):
            load = load + jnp.where(lane == expert_ref[s], totals[0][s : s + 1, :], 0.0)
        load_ref[...] = load * scale

    return local_call(
        body,
        [
            jax.ShapeDtypeStruct((owners * rows, padded), jnp.float32),
            jax.ShapeDtypeStruct((1, experts), jnp.float32),
        ],
        "gates",
        2 << 20,
        [pl.BlockSpec(memory_space=pltpu.VMEM)] * owners + [pl.BlockSpec(memory_space=pltpu.SMEM)],
    )(*infos, slot_expert)


def prepared(w_in):
    slots, width, two, units = w_in.shape
    tiles = units // LANES
    per_row = tiles * two
    block = width // 2
    part = WORK_ROWS
    interleaved = jnp.transpose(
        w_in.reshape(slots, width, two, tiles, LANES), (0, 1, 3, 2, 4)
    ).reshape(slots, width * per_row, LANES)

    def body(w_ref, first_ref, work):
        s, k = pl.program_id(0), pl.program_id(1)
        for u in range(block // part):
            spot = u % WORK_SLOTS
            work[spot] = w_ref[0, pl.ds(u * part * per_row, part * per_row)].astype(jnp.float32)
            rows = pl.ds(k * block + u * part, part)
            for j in range(tiles):
                for g in range(two):
                    first_ref[s, g, rows, j * LANES : (j + 1) * LANES] = work[
                        spot, pl.ds(two * j + g, part, stride=per_row), :
                    ].astype(jnp.bfloat16)

    return pl.pallas_call(
        body,
        grid=(slots, width // block),
        in_specs=[pl.BlockSpec((1, block * per_row, LANES), lambda s, k: (s, k, 0))],
        out_specs=pl.BlockSpec(memory_space=pltpu.VMEM),
        out_shape=pltpu.VMEM((slots, two, width, units), w_in.dtype),
        scratch_shapes=[pltpu.VMEM((WORK_SLOTS, part * per_row, LANES), jnp.float32)],
        compiler_params=pltpu.CompilerParams(
            dimension_semantics=("arbitrary", "arbitrary"), vmem_limit_bytes=9 << 20
        ),
        name="prepare",
    )(pltpu.with_memory_space_constraint(interleaved, pltpu.HBM))


def hidden_units(mine, theirs, gates, first):
    count = len(mine)
    rows, piece = mine[0].shape
    slots, _, _, units = first.shape

    def body(*refs):
        gate_ref, w_ref, out_ref, x_ref = refs[2 * count :]
        side = lax.axis_index("tensor")
        for i in range(count):
            x_ref[side, i * rows : (i + 1) * rows] = refs[i][...]
            x_ref[1 - side, i * rows : (i + 1) * rows] = refs[count + i][...]

        def product(s, g):
            return sum(
                jnp.dot(
                    x_ref[h],
                    w_ref[s, g, h * piece : (h + 1) * piece],
                    preferred_element_type=jnp.float32,
                )
                for h in range(2)
            )

        for s in range(slots):
            value = jax.nn.silu(product(s, 0)) * product(s, 1) * gate_ref[:, s : s + 1]
            out_ref[:, s * units : (s + 1) * units] = value.astype(out_ref.dtype)

    return local_call(
        body,
        pltpu.VMEM((count * rows, slots * units), first.dtype),
        "hidden",
        4 << 20,
        scratch=[pltpu.VMEM((2, count * rows, piece), first.dtype)],
    )(*mine, *theirs, gates, first)


def output_half(hidden, second, opposite, pieces):
    rows = hidden.shape[0] // pieces
    half = second.shape[1] // 2
    step = 2 * LANES if half % (2 * LANES) == 0 else LANES

    def body(h_ref, w_ref, *outs):
        side = lax.axis_index("tensor")
        which = 1 - side if opposite else side
        for first in range(0, half, step):
            cols = pl.ds(pl.multiple_of(which * half + first, LANES), step)
            value = jnp.dot(h_ref[...], w_ref[:, cols], preferred_element_type=jnp.float32)
            for i, out in enumerate(outs):
                part = value[i * rows : (i + 1) * rows]
                out[:, first : first + step] = part.astype(out.dtype)

    shapes = [jax.ShapeDtypeStruct((rows, half), hidden.dtype)] * pieces
    return local_call(body, shapes, "output", 4 << 20)(hidden, second)


def total(*values):
    def body(*refs):
        refs[-1][...] = sum(r[...].astype(jnp.float32) for r in refs[:-1]).astype(refs[-1].dtype)

    shape = jax.ShapeDtypeStruct(values[0].shape, values[0].dtype)
    return local_call(body, shape, "total", 2 << 20)(*values)


def gathered_plan(tokens, route_slots, route_scores, slot_expert, w_in, w_out):
    slot_local = w_in.shape[0]
    owners = lax.axis_size("expert")
    info = packed_routes(route_slots.T, route_scores.T)
    mine = gathered(tokens, "expert")
    infos = gathered(info, "expert")
    theirs = [swap(v, "tensor", 1) for v in mine]
    first = prepared(w_in)
    second = pltpu.with_memory_space_constraint(
        w_out.reshape(-1, w_out.shape[2]), pltpu.VMEM
    )
    gates, load = gates_and_load(infos, slot_expert, slot_local)
    hidden = hidden_units(mine, theirs, gates, first)
    give = output_half(hidden, second, True, owners)
    got = [swap(v, "tensor", 1) for v in give]
    keep = output_half(hidden, second, False, owners)
    terms = [[k, g] for k, g in zip(keep, got)]
    for bit in reversed(bits_of("expert")):
        for mask in reversed(range(owners)):
            if mask & bit and terms[mask]:
                terms[mask ^ bit].append(swap(total(*terms[mask]), "expert", bit))
                terms[mask] = []
    return total(*terms[0]), load


def shards(*args):
    tokens, route_slots, w_in = args[0], args[1], args[4]
    owners = lax.axis_size("expert")
    slot_count = w_in.shape[0] * owners
    capacity = 9 * tokens.shape[0] * route_slots.shape[1] // (8 * slot_count)
    dense = w_in.shape[0] * capacity >= tokens.shape[0]
    paired = owners & (owners - 1) == 0 and lax.axis_size("tensor") == 2
    return (gathered_plan if dense and paired else routed_plan)(*args)


def solution(mesh):
    placed = (
        P(("dp", "expert"), "tensor"),
        P(("dp", "expert"), None),
        P(("dp", "expert"), None),
        P(),
        P("expert", None, None, "tensor"),
        P("expert", "tensor", None),
    )
    return jax.shard_map(
        shards,
        mesh=mesh,
        in_specs=placed,
        out_specs=(P(("dp", "expert"), "tensor"), P("dp", None)),
        check_vma=False,
    )
```
